256 devices in a mesh: parts: 4 (over x, y), shard: 64 (over z, core).
Axes of the slice: x: 2, y: 2, z: 32, core: 2. Of those that a mesh axis runs over, the one named last changes fastest.
The devices are a block of a 4x8x32 slice.
Arguments:
- queries: bfloat16 [2048, 32, 128], P(('parts', 'shard')), parts along dimension 0, may hold values from -6 to 6
- doc_tokens: bfloat16 [2048, 128, 128], P(('parts', 'shard')), parts along dimension 0, may hold values from -0.5 to 0.5
- doc_lens: int32 [2048], P(('parts', 'shard')), parts along dimension 0, may hold values from 1 to 128
- candidates: int32 [2048, 128], P(('parts', 'shard')), parts along dimension 0, may hold values from 0 to 511
Outputs:
- scores: float32 [2048, 128], P(('parts', 'shard')), parts along dimension 0
The draws below stay inside these ranges and needn't reach their ends.
There are 4 independent parts, one for each index of `parts`. The reference program is written for one: setup_inputs(seed, part) draws one part's arguments, and reference() takes and returns one part's arrays. A program takes and returns all parts, laid end to end along the dimension named above; each array names one. Nothing has to cross between parts.
Inputs may be any that keep to these rules, and one draw needn't show every extreme that they name: `doc_lens`: every document has at least one live row. `candidates`: ids of documents of the same part.
All inputs are finite; a program needn't handle non-finite values.
Results may differ from the reference program's by a relative error of at most 0.0003.
Values may be sent and summed in bfloat16 or wider, within the bound.
No kernel may reach another device: no remote copies, remote signals or barrier semaphores. Data moves between devices by JAX's collectives and lax.ppermute only.
A program may use at most 64 MiB of HBM per device.

```python
import jax
import jax.numpy as jnp
from jax import lax

D = 128
QTOK = 32
BLOCK = 128
CAND = 128
QUERIES = 512
DOCS = 512


def touch_ends(result, key, low, largest):
    place = [jax.random.randint(jax.random.fold_in(key, axis), (), 0, length) for axis, length in enumerate(result.shape)]
    main_axis = result.shape.index(max(result.shape))
    next_to = place[:main_axis] + [(place[main_axis] + 1) % result.shape[main_axis]] + place[main_axis + 1:]
    return result.at[tuple(place)].set(low).at[tuple(next_to)].set(largest)


def steps_of(stream_key, dims, cuts, low, largest):
    def one(dim, blocks):
        draws = jax.random.uniform(jax.random.fold_in(jax.random.fold_in(stream_key, 6), dim), (blocks,), jnp.float32, low / len(cuts), largest / len(cuts))
        return jnp.repeat(jnp.exp(draws), dims[dim] // blocks).reshape((-1,) + (1,) * (len(dims) - dim - 1))

    factor_of = one(*cuts[0])
    for cut in cuts[1:]:
        factor_of = factor_of * one(*cut)
    return factor_of


def bell_draw(key, extent, spread, limit, pieces=(), kind=jnp.bfloat16):
    values = jax.random.normal(key, extent, jnp.float32) * spread
    if len(pieces) > 0:
        values = steps_of(key, extent, pieces, -0.22, 0.18) * values
    return jnp.clip(values, min=-limit, max=limit).astype(kind)


def setup_inputs(seed: int = 0, part: int = 0) -> dict:
    key_list = jax.random.split(jax.random.key(seed), 5)
    part_keys = jax.random.split(jax.random.fold_in(key_list[4], part), 5)
    queries = bell_draw(part_keys[0], (QUERIES, QTOK, D), 1.0, 6.0, ((0, 64),))
    doc_tokens = bell_draw(part_keys[1], (DOCS, BLOCK, D), D ** -0.5, 0.5, ((0, 64),))
    doc_lens = touch_ends(jax.random.randint(part_keys[2], (DOCS,), 1, BLOCK + 1), jax.random.fold_in(part_keys[2], 1), 1, BLOCK).astype(jnp.int32)
    candidates = touch_ends(jax.random.randint(part_keys[3], (QUERIES, CAND), 0, DOCS), jax.random.fold_in(part_keys[3], 1), 0, DOCS - 1).astype(jnp.int32)
    return dict(queries=queries, doc_tokens=doc_tokens, doc_lens=doc_lens, candidates=candidates)


def reference(queries, doc_tokens, doc_lens, candidates):
    rows = jnp.arange(doc_tokens.shape[1], dtype=jnp.int32)

    def one_query(item):
        query, picked = item
        blocks = doc_tokens[picked].astype(jnp.float32)
        live = rows[None, :] < doc_lens[picked][:, None]
        sim = jnp.einsum("id,cjd->cij", query.astype(jnp.float32), blocks)
        sim = jnp.where(live[:, None, :], sim, -1e30)
        return jnp.mean(jnp.max(sim, axis=2), axis=1)

    return lax.map(one_query, (queries, candidates))
```

```python
import functools

import jax
import jax.numpy as jnp
from jax import lax
from jax.experimental import pallas as pl
from jax.experimental.pallas import tpu as pltpu
from jax.sharding import PartitionSpec as P


AXIS = "shard"
SPEC = ("parts", "shard")
QTOK = 32
LANES = 128
HOPS = ((7, 6), (7, 5))
REACH = 3


def moved(value, up, down):
    size = lax.axis_size(AXIS)
    return lax.ppermute(value, AXIS, [(i, (i + (2 * up if i % 2 else -2 * down)) % size) for i in range(size)])


def crossed(value):
    size = lax.axis_size(AXIS)
    return lax.ppermute(value, AXIS, [(i, (i + (-3 if i % 2 else 3)) % size) for i in range(size)])


def swapped(value):
    size = lax.axis_size(AXIS)
    return lax.ppermute(value, AXIS, [(i, i ^ 1) for i in range(size)])


def in_vmem(count):
    return [pl.BlockSpec(memory_space=pltpu.VMEM)] * count


def fill_kernel(lens_ref, docs_ref, out_ref):
    count, rows, width = docs_ref.shape
    at = lax.broadcasted_iota(jnp.int32, (rows, width), 0)
    for k in range(count):
        block = docs_ref[k].astype(jnp.float32)
        out_ref[k * rows : (k + 1) * rows] = jnp.where(at < lens_ref[k], block, block[:1]).astype(out_ref.dtype)


def filled(docs, lens):
    count, rows, width = docs.shape
    return pl.pallas_call(
        fill_kernel,
        out_shape=jax.ShapeDtypeStruct((count * rows, width), docs.dtype),
        in_specs=[pl.BlockSpec(memory_space=pltpu.SMEM)] + in_vmem(1),
        out_specs=in_vmem(1)[0],
        cost_estimate=pl.CostEstimate(flops=1000000, bytes_accessed=0, transcendentals=0),
        compiler_params=pltpu.CompilerParams(vmem_limit_bytes=4 * 1024 * 1024),
    )(lens, docs)


def score_kernel(blocks, sets, carried, doc_rows, *refs):
    query_refs, doc_refs = refs[:blocks], refs[blocks : blocks + sets]
    old_refs, out_refs = refs[blocks + sets : -blocks], refs[-blocks:]
    for query_ref, out_ref, old in zip(query_refs, out_refs, old_refs or (None,) * blocks):
        rows = query_ref.shape[0]
        lane = lax.broadcasted_iota(jnp.int32, (rows, LANES), 1)
        pick = (lax.broadcasted_iota(jnp.int32, (rows, LANES), 0) // QTOK) == lane % 16
        pick = jnp.where(pick, 1.0 / QTOK, 0.0).astype(jnp.bfloat16)
        own = (lax.broadcasted_iota(jnp.int32, (8, LANES), 1) // 16) == lax.broadcasted_iota(jnp.int32, (8, LANES), 0)
        best = []
        for half in range(0, rows, 256):
            query = query_ref[half : half + 256]
            high = []
            for doc_ref in doc_refs:
                for at in range(0, doc_ref.shape[0], doc_rows):
                    sim = lax.dot_general(
                        doc_ref[at : at + doc_rows, :],
                        query,
                        (((1,), (1,)), ((), ())),
                        preferred_element_type=jnp.float32,
                    )
                    high.append(jnp.max(sim, axis=0, keepdims=True))
            best.append(jnp.concatenate(high, axis=0))
        best = jnp.concatenate(best, axis=1)
        first = best.astype(jnp.bfloat16)
        rest = best - first.astype(jnp.float32)
        second = rest.astype(jnp.bfloat16)
        third = (rest - second.astype(jnp.float32)).astype(jnp.bfloat16)
        mean = sum(jnp.dot(term, pick, preferred_element_type=jnp.float32) for term in (third, second, first))
        mean = jnp.where(own[None], mean.reshape(-1, 8, LANES), 0.0)
        if carried:
            out_ref[:carried] = old[...]
        out_ref[carried:] = jnp.sum(mean, axis=1)


def scored(queries, docs, old, doc_rows):
    blocks, sets = len(queries), len(docs)
    width = queries[0].shape[1]
    flops = 2 * sum(q.shape[0] for q in queries) * sum(d.shape[0] for d in docs) * width
    carried = old[0].shape[0] if old else 0
    return pl.pallas_call(
        functools.partial(score_kernel, blocks, sets, carried, doc_rows),
        out_shape=[jax.ShapeDtypeStruct((carried + 2 * sets, LANES), jnp.float32)] * blocks,
        in_specs=in_vmem(blocks + sets + len(old)),
        out_specs=in_vmem(blocks),
        cost_estimate=pl.CostEstimate(flops=flops, bytes_accessed=0, transcendentals=0),
        compiler_params=pltpu.CompilerParams(vmem_limit_bytes=16 * 1024 * 1024),
    )(*queries, *docs, *old)


def pick_kernel(up_parts, down_parts, count, chips, *refs):
    block_refs, (candidates_ref, out_ref) = refs[:-2], refs[-2:]
    me = lax.axis_index(AXIS)
    core = lax.rem(me, 2)

    def line_of(block, row, theirs):
        line = block_refs[block][row : row + 1]
        return jnp.concatenate([line[:, 8:], line[:, :8]], axis=1) if theirs else line

    rows = []
    for up, down in zip(up_parts, down_parts):
        line = line_of(*up)
        rows.append(line if up == down else jnp.where(core == 1, line, line_of(*down)))
    rows.append(jnp.zeros((LANES - len(rows), LANES), jnp.float32))
    table = jnp.concatenate(rows, axis=0).T
    wanted = candidates_ref[...]
    holder = lax.div(wanted, count)
    doc = wanted - count * holder
    side = lax.rem(holder + core, 2)
    away = (lax.div(holder, 2) - lax.div(me, 2)) * (2 * core - 1)
    row = 2 * lax.rem(away + (chips + chips // 2 - 1), chips) + side
    result = jnp.zeros(out_ref.shape, jnp.float32)
    for j in range(count):
        line = jnp.take_along_axis(table[16 * j : 16 * j + 8], row, axis=1, mode="promise_in_bounds")
        result = jnp.where(doc == j, line, result)
    out_ref[...] = result


def picked(blocks, up_parts, down_parts, candidates, count, chips):
    return pl.pallas_call(
        functools.partial(pick_kernel, up_parts, down_parts, count, chips),
        out_shape=jax.ShapeDtypeStruct(candidates.shape, jnp.float32),
        in_specs=in_vmem(len(blocks) + 1),
        out_specs=in_vmem(1)[0],
        cost_estimate=pl.CostEstimate(flops=100000, bytes_accessed=0, transcendentals=0),
        compiler_params=pltpu.CompilerParams(vmem_limit_bytes=4 * 1024 * 1024),
    )(*blocks, candidates)


def body(queries, doc_tokens, doc_lens, candidates):
    chips = lax.axis_size(AXIS) // 2
    count, rows, width = doc_tokens.shape
    query = queries.reshape(-1, width)
    docs = filled(doc_tokens, doc_lens)

    both = jnp.concatenate([query, swapped(query)], axis=0)
    places = [query]
    for up, down in zip(*HOPS):
        both = moved(both, up, down)
        places.append(both)
    near = {0: jnp.concatenate([docs, swapped(docs)], axis=0)}
    for step in range(REACH):
        if step == 0:
            held = jnp.concatenate([moved(docs, 1, 1), crossed(docs)], axis=0)
        else:
            held = moved(held, 1, 1)
        near[-step - 1] = held
        near[step + 1] = swapped(held)

    stops = [[sum(hops[:k]) for k in range(len(hops) + 1)] for hops in HOPS]
    half = chips // 2
    plan = []
    for away in range(1 - half, half + 1):
        way = stops[away < 0]
        stop = min(range(len(way)), key=lambda k: abs(abs(away) - way[k]))
        plan.append((away, stop, (away if stop == 0 else abs(away)) - way[stop]))

    offsets = [() for _ in places]
    result = [None for _ in places]
    far = range(2, len(places))
    last = sorted({o for _, stop, o in plan if stop in far})
    for group, added in (((0, 1), (0, -1, 1)), ((0, 1), (-2, 2)), ((0, 1), (-3,)), ((0, 1), (3,)), (far, last)):
        old = [result[k] for k in group if result[k] is not None]
        outs = scored([places[k] for k in group], [near[o] for o in added], old, rows)
        for k, out in zip(group, outs):
            result[k] = out
            offsets[k] += tuple(added)

    blocks = [result[0]]
    for k in range(1, len(places)):
        mine = moved(result[k], -stops[0][k], -stops[1][k])
        blocks += [mine, swapped(mine)]

    def parts_of(core):
        found = {}
        for away, stop, o in plan:
            theirs = stop > 0 and (away < 0) == (core == 1)
            mine = away if core == 1 else -away
            o = mine if stop == 0 else o
            for side in range(2):
                first = side ^ (o > 0) ^ theirs
                block = 0 if stop == 0 else 2 * stop - 1 + theirs
                found[(mine + half - 1) % chips, side] = (block, 2 * offsets[stop].index(o) + first, theirs)
        return [found[at, side] for at in range(chips) for side in range(2)]

    return picked(blocks, parts_of(1), parts_of(0), candidates, count, chips)


def solution(mesh):
    return jax.shard_map(
        body,
        mesh=mesh,
        in_specs=(P(SPEC, None, None), P(SPEC, None, None), P(SPEC), P(SPEC, None)),
        out_specs=P(SPEC, None),
        check_vma=False,
    )
```

```python
import functools

import jax
import jax.numpy as jnp
from jax import lax
from jax.experimental import pallas as pl
from jax.experimental.pallas import tpu as pltpu
from jax.sharding import PartitionSpec as P


AXIS = "shard"
SPEC = ("parts", "shard")
QTOK = 32
LANES = 128
HOPS = ((7, 6), (6, 6))
REACH = 3


def moved(value, up, down):
    size = lax.axis_size(AXIS)
    return lax.ppermute(value, AXIS, [(i, (i + (2 * up if i % 2 else -2 * down)) % size) for i in range(size)])


def crossed(value):
    size = lax.axis_size(AXIS)
    return lax.ppermute(value, AXIS, [(i, (i + (-3 if i % 2 else 3)) % size) for i in range(size)])


def swapped(value):
    size = lax.axis_size(AXIS)
    return lax.ppermute(value, AXIS, [(i, i ^ 1) for i in range(size)])


def in_vmem(count):
    return [pl.BlockSpec(memory_space=pltpu.VMEM)] * count


def fill_kernel(lens_ref, docs_ref, out_ref):
    count, rows, width = docs_ref.shape
    at = lax.broadcasted_iota(jnp.int32, (rows, width), 0)
    for k in range(count):
        block = docs_ref[k].astype(jnp.float32)
        out_ref[k * rows : (k + 1) * rows] = jnp.where(at < lens_ref[k], block, block[:1]).astype(out_ref.dtype)


def filled(docs, lens):
    count, rows, width = docs.shape
    return pl.pallas_call(
        fill_kernel,
        out_shape=jax.ShapeDtypeStruct((count * rows, width), docs.dtype),
        in_specs=[pl.BlockSpec(memory_space=pltpu.SMEM)] + in_vmem(1),
        out_specs=in_vmem(1)[0],
        cost_estimate=pl.CostEstimate(flops=1000000, bytes_accessed=0, transcendentals=0),
        compiler_params=pltpu.CompilerParams(vmem_limit_bytes=4 * 1024 * 1024),
    )(lens, docs)


def score_kernel(blocks, sets, carried, doc_rows, *refs):
    query_refs, doc_refs = refs[:blocks], refs[blocks : blocks + sets]
    old_refs, out_refs = refs[blocks + sets : -blocks], refs[-blocks:]
    for query_ref, out_ref, old in zip(query_refs, out_refs, old_refs or (None,) * blocks):
        rows = query_ref.shape[0]
        lane = lax.broadcasted_iota(jnp.int32, (rows, LANES), 1)
        pick = (lax.broadcasted_iota(jnp.int32, (rows, LANES), 0) // QTOK) == lane % 16
        pick = jnp.where(pick, 1.0 / QTOK, 0.0).astype(jnp.bfloat16)
        own = (lax.broadcasted_iota(jnp.int32, (8, LANES), 1) // 16) == lax.broadcasted_iota(jnp.int32, (8, LANES), 0)
        best = []
        for half in range(0, rows, 256):
            query = query_ref[half : half + 256]
            high = []
            for doc_ref in doc_refs:
                for at in range(0, doc_ref.shape[0], doc_rows):
                    sim = lax.dot_general(
                        doc_ref[at : at + doc_rows, :],
                        query,
                        (((1,), (1,)), ((), ())),
                        preferred_element_type=jnp.float32,
                    )
                    high.append(jnp.max(sim, axis=0, keepdims=True))
            best.append(jnp.concatenate(high, axis=0))
        best = jnp.concatenate(best, axis=1)
        first = best.astype(jnp.bfloat16)
        rest = best - first.astype(jnp.float32)
        second = rest.astype(jnp.bfloat16)
        third = (rest - second.astype(jnp.float32)).astype(jnp.bfloat16)
        mean = sum(jnp.dot(term, pick, preferred_element_type=jnp.float32) for term in (third, second, first))
        mean = jnp.where(own[None], mean.reshape(-1, 8, LANES), 0.0)
        if carried:
            out_ref[:carried] = old[...]
        out_ref[carried:] = jnp.sum(mean, axis=1)


def scored(queries, docs, old, doc_rows):
    blocks, sets = len(queries), len(docs)
    width = queries[0].shape[1]
    flops = 2 * sum(q.shape[0] for q in queries) * sum(d.shape[0] for d in docs) * width
    carried = old[0].shape[0] if old else 0
    return pl.pallas_call(
        functools.partial(score_kernel, blocks, sets, carried, doc_rows),
        out_shape=[jax.ShapeDtypeStruct((carried + 2 * sets, LANES), jnp.float32)] * blocks,
        in_specs=in_vmem(blocks + sets + len(old)),
        out_specs=in_vmem(blocks),
        cost_estimate=pl.CostEstimate(flops=flops, bytes_accessed=0, transcendentals=0),
        compiler_params=pltpu.CompilerParams(vmem_limit_bytes=16 * 1024 * 1024),
    )(*queries, *docs, *old)


def pick_kernel(up_parts, down_parts, count, chips, *refs):
    block_refs, (candidates_ref, out_ref) = refs[:-2], refs[-2:]
    me = lax.axis_index(AXIS)
    core = lax.rem(me, 2)

    def line_of(block, row, theirs):
        line = block_refs[block][row : row + 1]
        return jnp.concatenate([line[:, 8:], line[:, :8]], axis=1) if theirs else line

    rows = []
    for up, down in zip(up_parts, down_parts):
        line = line_of(*up)
        rows.append(line if up == down else jnp.where(core == 1, line, line_of(*down)))
    rows.append(jnp.zeros((LANES - len(rows), LANES), jnp.float32))
    table = jnp.concatenate(rows, axis=0).T
    wanted = candidates_ref[...]
    holder = lax.div(wanted, count)
    doc = wanted - count * holder
    side = lax.rem(holder + core, 2)
    away = (lax.div(holder, 2) - lax.div(me, 2)) * (2 * core - 1)
    row = 2 * lax.rem(away + (chips + chips // 2 - 1), chips) + side
    result = jnp.zeros(out_ref.shape, jnp.float32)
    for j in range(count):
        line = jnp.take_along_axis(table[16 * j : 16 * j + 8], row, axis=1, mode="promise_in_bounds")
        result = jnp.where(doc == j, line, result)
    out_ref[...] = result


def picked(blocks, up_parts, down_parts, candidates, count, chips):
    return pl.pallas_call(
        functools.partial(pick_kernel, up_parts, down_parts, count, chips),
        out_shape=jax.ShapeDtypeStruct(candidates.shape, jnp.float32),
        in_specs=in_vmem(len(blocks) + 1),
        out_specs=in_vmem(1)[0],
        cost_estimate=pl.CostEstimate(flops=100000, bytes_accessed=0, transcendentals=0),
        compiler_params=pltpu.CompilerParams(vmem_limit_bytes=4 * 1024 * 1024),
    )(*blocks, candidates)


def body(queries, doc_tokens, doc_lens, candidates):
    chips = lax.axis_size(AXIS) // 2
    count, rows, width = doc_tokens.shape
    query = queries.reshape(-1, width)
    docs = filled(doc_tokens, doc_lens)

    both = jnp.concatenate([query, swapped(query)], axis=0)
    places = [query]
    for up, down in zip(*HOPS):
        both = moved(both, up, down)
        places.append(both)
    near = {0: jnp.concatenate([docs, swapped(docs)], axis=0)}
    for step in range(REACH):
        if step == 0:
            held = jnp.concatenate([moved(docs, 1, 1), crossed(docs)], axis=0)
        else:
            held = moved(held, 1, 1)
        near[-step - 1] = held
        near[step + 1] = swapped(held)

    stops = [[sum(hops[:k]) for k in range(len(hops) + 1)] for hops in HOPS]
    half = chips // 2
    plan = []
    for away in range(1 - half, half + 1):
        way = stops[away < 0]
        stop = min(range(len(way)), key=lambda k: abs(abs(away) - way[k]))
        plan.append((away, stop, (away if stop == 0 else abs(away)) - way[stop]))

    offsets = [() for _ in places]
    result = [None for _ in places]
    far = range(2, len(places))
    last = sorted({o for _, stop, o in plan if stop in far})
    for group, added in (
        ((0, 1), (0, -1, 1)),
        ((0, 1), (-2, 2)),
        (far, tuple(o for o in last if abs(o) < REACH)),
        (far, tuple(o for o in last if abs(o) == REACH)),
        ((1,), (-3,)),
        ((1,), (3,)),
        ((0,), (-3, 3)),
    ):
        old = [result[k] for k in group if result[k] is not None]
        outs = scored([places[k] for k in group], [near[o] for o in added], old, rows)
        for k, out in zip(group, outs):
            result[k] = out
            offsets[k] += tuple(added)

    blocks = [result[0]]
    for k in range(1, len(places)):
        mine = moved(result[k], -stops[0][k], -stops[1][k])
        blocks += [mine, swapped(mine)]

    def parts_of(core):
        found = {}
        for away, stop, o in plan:
            theirs = stop > 0 and (away < 0) == (core == 1)
            mine = away if core == 1 else -away
            o = mine if stop == 0 else o
            for side in range(2):
                first = side ^ (o > 0) ^ theirs
                block = 0 if stop == 0 else 2 * stop - 1 + theirs
                found[(mine + half - 1) % chips, side] = (block, 2 * offsets[stop].index(o) + first, theirs)
        return [found[at, side] for at in range(chips) for side in range(2)]

    return picked(blocks, parts_of(1), parts_of(0), candidates, count, chips)


def solution(mesh):
    return jax.shard_map(
        body,
        mesh=mesh,
        in_specs=(P(SPEC, None, None), P(SPEC, None, None), P(SPEC), P(SPEC, None)),
        out_specs=P(SPEC, None),
        check_vma=False,
    )
```

```python
import functools

import jax
import jax.numpy as jnp
from jax import lax
from jax.experimental import pallas as pl
from jax.experimental.pallas import tpu as pltpu
from jax.sharding import PartitionSpec as P


AXIS = "shard"
SPEC = ("parts", "shard")
QTOK = 32
LANES = 128
HOPS = ((7, 6), (6, 6))
REACH = 3


def moved(value, up, down):
    size = lax.axis_size(AXIS)
    return lax.ppermute(value, AXIS, [(i, (i + (2 * up if i % 2 else -2 * down)) % size) for i in range(size)])


def crossed(value):
    size = lax.axis_size(AXIS)
    return lax.ppermute(value, AXIS, [(i, (i + (-3 if i % 2 else 3)) % size) for i in range(size)])


def handed(value):
    size = lax.axis_size(AXIS)
    return lax.ppermute(value, AXIS, [(i, (i + (1 if i % 2 else -1)) % size) for i in range(size)])


def swapped(value):
    size = lax.axis_size(AXIS)
    return lax.ppermute(value, AXIS, [(i, i ^ 1) for i in range(size)])


def in_vmem(count):
    return [pl.BlockSpec(memory_space=pltpu.VMEM)] * count


def fill_kernel(lens_ref, docs_ref, out_ref):
    count, rows, width = docs_ref.shape
    at = lax.broadcasted_iota(jnp.int32, (rows, width), 0)
    for k in range(count):
        block = docs_ref[k].astype(jnp.float32)
        out_ref[k * rows : (k + 1) * rows] = jnp.where(at < lens_ref[k], block, block[:1]).astype(out_ref.dtype)


def filled(docs, lens):
    count, rows, width = docs.shape
    return pl.pallas_call(
        fill_kernel,
        out_shape=jax.ShapeDtypeStruct((count * rows, width), docs.dtype),
        in_specs=[pl.BlockSpec(memory_space=pltpu.SMEM)] + in_vmem(1),
        out_specs=in_vmem(1)[0],
        cost_estimate=pl.CostEstimate(flops=1000000, bytes_accessed=0, transcendentals=0),
        compiler_params=pltpu.CompilerParams(vmem_limit_bytes=4 * 1024 * 1024),
    )(lens, docs)


def score_kernel(blocks, sets, carried, doc_rows, *refs):
    query_refs, doc_refs = refs[:blocks], refs[blocks : blocks + sets]
    old_refs, out_refs = refs[blocks + sets : -blocks], refs[-blocks:]
    for query_ref, out_ref, old in zip(query_refs, out_refs, old_refs or (None,) * blocks):
        rows = query_ref.shape[0]
        lane = lax.broadcasted_iota(jnp.int32, (rows, LANES), 1)
        pick = (lax.broadcasted_iota(jnp.int32, (rows, LANES), 0) // QTOK) == lane % 16
        pick = jnp.where(pick, 1.0 / QTOK, 0.0).astype(jnp.bfloat16)
        own = (lax.broadcasted_iota(jnp.int32, (8, LANES), 1) // 16) == lax.broadcasted_iota(jnp.int32, (8, LANES), 0)
        best = []
        for half in range(0, rows, 256):
            query = query_ref[half : half + 256]
            high = []
            for doc_ref in doc_refs:
                for at in range(0, doc_ref.shape[0], doc_rows):
                    sim = lax.dot_general(
                        doc_ref[at : at + doc_rows, :],
                        query,
                        (((1,), (1,)), ((), ())),
                        preferred_element_type=jnp.float32,
                    )
                    high.append(jnp.max(sim, axis=0, keepdims=True))
            best.append(jnp.concatenate(high, axis=0))
        best = jnp.concatenate(best, axis=1)
        first = best.astype(jnp.bfloat16)
        rest = best - first.astype(jnp.float32)
        second = rest.astype(jnp.bfloat16)
        third = (rest - second.astype(jnp.float32)).astype(jnp.bfloat16)
        mean = sum(jnp.dot(term, pick, preferred_element_type=jnp.float32) for term in (third, second, first))
        mean = jnp.where(own[None], mean.reshape(-1, 8, LANES), 0.0)
        if carried:
            out_ref[:carried] = old[...]
        out_ref[carried:] = jnp.sum(mean, axis=1)


def scored(queries, docs, old, doc_rows):
    blocks, sets = len(queries), len(docs)
    width = queries[0].shape[1]
    flops = 2 * sum(q.shape[0] for q in queries) * sum(d.shape[0] for d in docs) * width
    carried = old[0].shape[0] if old else 0
    return pl.pallas_call(
        functools.partial(score_kernel, blocks, sets, carried, doc_rows),
        out_shape=[jax.ShapeDtypeStruct((carried + 2 * sets, LANES), jnp.float32)] * blocks,
        in_specs=in_vmem(blocks + sets + len(old)),
        out_specs=in_vmem(blocks),
        cost_estimate=pl.CostEstimate(flops=flops, bytes_accessed=0, transcendentals=0),
        compiler_params=pltpu.CompilerParams(vmem_limit_bytes=16 * 1024 * 1024),
    )(*queries, *docs, *old)


def pick_kernel(up_parts, down_parts, count, chips, *refs):
    block_refs, (candidates_ref, out_ref) = refs[:-2], refs[-2:]
    me = lax.axis_index(AXIS)
    core = lax.rem(me, 2)

    def line_of(block, row, theirs):
        line = block_refs[block][row : row + 1]
        return jnp.concatenate([line[:, 8:], line[:, :8]], axis=1) if theirs else line

    rows = []
    for up, down in zip(up_parts, down_parts):
        line = line_of(*up)
        rows.append(line if up == down else jnp.where(core == 1, line, line_of(*down)))
    rows.append(jnp.zeros((LANES - len(rows), LANES), jnp.float32))
    table = jnp.concatenate(rows, axis=0).T
    wanted = candidates_ref[...]
    holder = lax.div(wanted, count)
    doc = wanted - count * holder
    side = lax.rem(holder + core, 2)
    away = (lax.div(holder, 2) - lax.div(me, 2)) * (2 * core - 1)
    row = 2 * lax.rem(away + (chips + chips // 2 - 1), chips) + side
    result = jnp.zeros(out_ref.shape, jnp.float32)
    for j in range(count):
        line = jnp.take_along_axis(table[16 * j : 16 * j + 8], row, axis=1, mode="promise_in_bounds")
        result = jnp.where(doc == j, line, result)
    out_ref[...] = result


def picked(blocks, up_parts, down_parts, candidates, count, chips):
    return pl.pallas_call(
        functools.partial(pick_kernel, up_parts, down_parts, count, chips),
        out_shape=jax.ShapeDtypeStruct(candidates.shape, jnp.float32),
        in_specs=in_vmem(len(blocks) + 1),
        out_specs=in_vmem(1)[0],
        cost_estimate=pl.CostEstimate(flops=100000, bytes_accessed=0, transcendentals=0),
        compiler_params=pltpu.CompilerParams(vmem_limit_bytes=4 * 1024 * 1024),
    )(*blocks, candidates)


def body(queries, doc_tokens, doc_lens, candidates):
    chips = lax.axis_size(AXIS) // 2
    count, rows, width = doc_tokens.shape
    query = queries.reshape(-1, width)
    docs = filled(doc_tokens, doc_lens)

    both = jnp.concatenate([query, swapped(query)], axis=0)
    places = [query]
    for up, down in zip(*HOPS):
        both = moved(both, up, down)
        places.append(both)
    near = {0: jnp.concatenate([docs, swapped(docs)], axis=0)}
    held = jnp.concatenate([moved(docs, 1, 1), crossed(docs)], axis=0)
    near[-1], near[1] = held, swapped(held)
    for step in range(1, REACH - 1):
        held = moved(held, 1, 1)
        near[-step - 1], near[step + 1] = held, swapped(held)
    near[REACH] = handed(held)
    near[-REACH] = swapped(near[REACH])

    stops = [[sum(hops[:k]) for k in range(len(hops) + 1)] for hops in HOPS]
    half = chips // 2
    plan = []
    for away in range(1 - half, half + 1):
        way = stops[away < 0]
        stop = min(range(len(way)), key=lambda k: abs(abs(away) - way[k]))
        plan.append((away, stop, (away if stop == 0 else abs(away)) - way[stop]))

    offsets = [() for _ in places]
    result = [None for _ in places]
    far = range(2, len(places))
    last = sorted({o for _, stop, o in plan if stop in far})
    for group, added in (
        ((0, 1), (0, -1, 1)),
        ((0, 1), (-2, 2)),
        (far, tuple(o for o in last if abs(o) < REACH)),
        (far, tuple(o for o in last if abs(o) == REACH)),
        ((1,), (-3, 3)),
        ((0,), (-3, 3)),
    ):
        old = [result[k] for k in group if result[k] is not None]
        outs = scored([places[k] for k in group], [near[o] for o in added], old, rows)
        for k, out in zip(group, outs):
            result[k] = out
            offsets[k] += tuple(added)

    blocks = [result[0]]
    for k in range(1, len(places)):
        mine = moved(result[k], -stops[0][k], -stops[1][k])
        blocks += [mine, swapped(mine)]

    def parts_of(core):
        found = {}
        for away, stop, o in plan:
            theirs = stop > 0 and (away < 0) == (core == 1)
            mine = away if core == 1 else -away
            o = mine if stop == 0 else o
            for side in range(2):
                first = side ^ (o > 0) ^ theirs
                block = 0 if stop == 0 else 2 * stop - 1 + theirs
                found[(mine + half - 1) % chips, side] = (block, 2 * offsets[stop].index(o) + first, theirs)
        return [found[at, side] for at in range(chips) for side in range(2)]

    return picked(blocks, parts_of(1), parts_of(0), candidates, count, chips)


def solution(mesh):
    return jax.shard_map(
        body,
        mesh=mesh,
        in_specs=(P(SPEC, None, None), P(SPEC, None, None), P(SPEC), P(SPEC, None)),
        out_specs=P(SPEC, None),
        check_vma=False,
    )
```
